32 devices in a mesh: slab: 16 (over z, y, x), comp: 2 (over core).
Axes of the slice: x: 2, y: 2, z: 4, core: 2. Of those that a mesh axis runs over, the one named last changes fastest.
Arguments:
- polarization: float32 [6, 16, 128, 128], P('comp', 'slab'), parts along dimension 0, may hold values from -6 to 6
- inverse_polarizability: float32 [16, 128, 128], P('slab'), may hold values from 0.5 to 2
- occupancy: int32 [16, 16, 16], P('slab'), may hold values 0 or 1
- green_fourier: float32 [6, 256, 32, 256], P(None, 'slab'), may hold values from -12 to 12
Outputs:
- first_image: float32 [6, 16, 128, 128], P('comp', 'slab'), parts along dimension 0
- second_image: float32 [6, 16, 128, 128], P('comp', 'slab'), parts along dimension 0
The draws below stay inside these ranges and needn't reach their ends.
There are 2 independent parts, one for each index of `comp`. The reference program is written for one: setup_inputs(seed, part) draws one part's arguments, and reference() takes and returns one part's arrays. A program takes and returns all parts, laid end to end along the dimension named above; an argument that names none is the same for every part. Nothing has to cross between parts.
All inputs are finite; a program needn't handle non-finite values. No bound on the sum of `occupancy` on one device may be relied on, other than what follows from the above.
Results may differ from the reference program's by a relative error of at most 0.0001.
Values sent between devices are 32-bit elements; how exact they have to be, the bound alone decides.
A program may use at most 64 MiB of HBM per device.

```python
import math
import jax
import jax.numpy as jnp

NY = 128
NZ = 128
BLOCK = 8
MATVECS = 2
NX = 16
LX = 32
LY = 256
LZ = 256


def plant(entries, own_key, smallest, largest):
    index_at = [jax.random.randint(jax.random.fold_in(own_key, axis), (), 0, length) for axis, length in enumerate(entries.shape)]
    main_axis = entries.shape.index(max(entries.shape))
    beside = index_at[:main_axis] + [(index_at[main_axis] + 1) % entries.shape[main_axis]] + index_at[main_axis + 1:]
    return entries.at[tuple(index_at)].set(smallest).at[tuple(beside)].set(largest)


def block_scale(own_key, dims, pieces, least, top_value):
    gain, own = 1.0, jax.random.fold_in(own_key, 6)
    for position, shards_of in pieces:
        heights = jnp.exp(jax.random.uniform(jax.random.fold_in(own, position), (shards_of,), jnp.float32, least / len(pieces), top_value / len(pieces)))
        gain = gain * jnp.repeat(heights, dims[position] // shards_of).reshape([-1 if axis == position else 1 for axis in range(len(dims))])
    return gain


def centred(key, extent, width, reach, shards=(), dtype=jnp.bfloat16):
    factor_of = block_scale(key, extent, shards, -0.22, 0.18) if shards else 1.0
    result = jax.random.normal(key, extent, jnp.float32) * width * factor_of
    return jnp.minimum(jnp.maximum(result, -reach), reach).astype(dtype)


def setup_inputs(seed: int = 0, part: int = 0) -> dict:
    arg_keys = jax.random.split(jax.random.key(seed), 5)
    part_splits = jax.random.split(jax.random.fold_in(arg_keys[4], part), 5)
    polarization = centred(part_splits[0], (3, NX, NY, NZ), 1.0, 6.0, ((1, 16),), jnp.float32)
    inverse_polarizability = jnp.clip(jnp.exp(math.log(2.0) - 1.3862944 * jax.random.uniform(arg_keys[1], (NX, NY, NZ), jnp.float32) ** block_scale(arg_keys[1], (NX, NY, NZ), ((0, 16),), -0.2, 0.2)), 0.5, 2.0)
    occupancy = plant((jax.random.randint(arg_keys[2], (NX, NY // BLOCK, NZ // BLOCK), 0, 4) < 3).astype(jnp.int32), jax.random.fold_in(arg_keys[2], 1), 0, 1)
    green_fourier = centred(arg_keys[3], (6, LZ, LX, LY), 2.0, 12.0, ((1, 16),), jnp.float32)
    return dict(polarization=polarization, inverse_polarizability=inverse_polarizability, occupancy=occupancy, green_fourier=green_fourier)


def expand_mask(occupancy):
    flags = occupancy.astype(jnp.float32)
    first, second, third = flags.shape
    spread = jnp.broadcast_to(flags[:, :, None, :, None], (first, second, BLOCK, third, BLOCK))
    return spread.reshape(first, second * BLOCK, third * BLOCK)


def apply_operator(field, mask, inverse_polarizability, green_ordered):
    masked = field * mask[None]
    padded = jnp.pad(masked, ((0, 0), (0, NX), (0, NY), (0, NZ)))
    spectrum = jnp.fft.fftn(padded, axes=(1, 2, 3))
    combos = ((0, 3, 4), (3, 1, 5), (4, 5, 2))
    results = []
    for row in combos:
        product = green_ordered[row[0]] * spectrum[0] + green_ordered[row[1]] * spectrum[1] + green_ordered[row[2]] * spectrum[2]
        back = jnp.fft.ifftn(product).real[:NX, :NY, :NZ]
        results.append(back.astype(jnp.float32))
    convolved = jnp.stack(results)
    return inverse_polarizability[None] * masked - mask[None] * convolved


def reference(polarization, inverse_polarizability, occupancy, green_fourier):
    mask = expand_mask(occupancy)
    green_ordered = jnp.transpose(green_fourier, (0, 2, 3, 1))
    first_image = apply_operator(polarization, mask, inverse_polarizability, green_ordered)
    current = first_image
    for repeat_index in range(MATVECS - 1):
        current = apply_operator(current, mask, inverse_polarizability, green_ordered)
    return first_image, current
```

```python
import functools
import math

import jax
import jax.numpy as jnp
import numpy as np
from jax import lax
from jax.experimental import pallas as pl
from jax.experimental.pallas import tpu as pltpu
from jax.sharding import PartitionSpec as P

BLOCK = 8
MATVECS = 2
F32 = jnp.float32
BF16 = jnp.bfloat16
COMBOS = ((0, 3, 4), (3, 1, 5), (4, 5, 2))


def tables(count_in, count_out, length):
    phase = np.arange(count_in)[:, None] * np.arange(count_out)[None, :] % length
    angle = phase * (2.0 * math.pi / length)
    return np.cos(angle), np.sin(angle)


def split_table(table):
    table = table.astype(np.float32)
    high = table.astype(jnp.bfloat16)
    low = (table - high.astype(np.float32)).astype(jnp.bfloat16)
    return high, low


def split(value):
    high = value.astype(BF16)
    return high, (value - high.astype(F32)).astype(BF16)


def twiddle(re, im, num, length, sign):
    num = num * sign % length
    if num == 0:
        return re, im
    if 4 * num == length:
        return -im, re
    if 2 * num == length:
        return -re, -im
    if 4 * num == 3 * length:
        return im, -re
    c = math.cos(2.0 * math.pi * num / length)
    s = math.sin(2.0 * math.pi * num / length)
    if (8 * num) % length == 0:
        a = abs(c)
        p, m = (re + im) * a, (re - im) * a
        return {1: (m, p), 3: (-p, m), 5: (-m, -p), 7: (p, -m)}[8 * num // length]
    return re * c - im * s, re * s + im * c


def fft(values, sign):
    n = len(values)
    if n == 1:
        return values
    even, odd = fft(values[0::2], sign), fft(values[1::2], sign)
    low, high = [], []
    for k in range(n // 2):
        (er, ei), (o_r, oi) = even[k], twiddle(*odd[k], k, n, sign)
        low.append((er + o_r, ei + oi))
        high.append((er - o_r, ei - oi))
    return low + high


def three_pass(pair, table_pair, dims):
    dot = functools.partial(lax.dot_general, dimension_numbers=dims, preferred_element_type=F32)
    (vh, vl), (th, tl) = pair, table_pair
    return dot(vh, th) + (dot(vl, th) + dot(vh, tl))


def kernel(
    n, cells_x, padded_x, kz_own, kc,
    pol_ref, inv_ref, occ_ref, green_ref, wz_h, wz_l, wy_h, wy_l, vy_h, vy_l, vz_h, vz_l,
    first_ref, second_ref,
    green_raw, green, mask_ref, out_t, in_t, spec, fld, out_u, in_u,
    green_sem, fs_sem, fr_sem, is_sem, ir_sem,
):
    me = lax.axis_index("slab")
    chunks = kz_own // kc
    cells_y, cells_z = mask_ref.shape
    padded_y = 2 * cells_y
    halves = padded_y // 128
    green_copy = pltpu.make_async_copy(green_ref, green_raw, green_sem)
    green_copy.start()

    barrier = pltpu.get_barrier_semaphore()

    def greet(k, carry):
        pl.semaphore_signal(
            barrier, inc=1, device_id={"slab": lax.rem(me + k, n)}, device_id_type=pl.DeviceIdType.MESH
        )
        return carry

    lax.fori_loop(1, n, greet, 0)

    blocks_y, blocks_z = occ_ref.shape[1:]
    up_y = lax.broadcasted_iota(jnp.int32, (cells_y, blocks_y), 0) // BLOCK
    up_y = (up_y == lax.broadcasted_iota(jnp.int32, (cells_y, blocks_y), 1)).astype(F32).astype(BF16)
    up_z = lax.broadcasted_iota(jnp.int32, (blocks_z, cells_z), 1) // BLOCK
    up_z = (up_z == lax.broadcasted_iota(jnp.int32, (blocks_z, cells_z), 0)).astype(F32).astype(BF16)
    flags = occ_ref[0].astype(F32).astype(BF16)
    spread = jnp.dot(up_y, flags, preferred_element_type=F32).astype(BF16)
    mask_ref[...] = jnp.dot(spread, up_z, preferred_element_type=F32)

    def forward_z(c, field):
        pair = split(field)
        for part in range(2):
            rows = slice(part * 2 * cells_z, (part + 1) * 2 * cells_z)
            dims = (((1,), (1,)), ((), ()))
            res = three_pass((wz_h[rows, :], wz_l[rows, :]), pair, dims)
            out_t[:, 2 * c + part] = res.reshape(n, kz_own, cells_y)

    def block(ref, index, j):
        return ref.at[index, :, pl.ds(j * kc, kc), :]

    def exchange(source, target, j, send_sem, recv_sem):
        def send(k, carry):
            peer = lax.rem(me + k, n)
            pltpu.make_async_remote_copy(
                src_ref=block(source, peer, j),
                dst_ref=block(target, me, j),
                send_sem=send_sem,
                recv_sem=recv_sem,
                device_id={"slab": peer},
                device_id_type=pl.DeviceIdType.MESH,
            ).start()
            return carry

        lax.fori_loop(1, n, send, 0)
        target[me, :, j * kc:(j + 1) * kc, :] = source[me, :, j * kc:(j + 1) * kc, :]

    def drain(ref, sem, j):
        view = ref.at[pl.ds(0, n - 1), :, pl.ds(j * kc, kc), :]
        pltpu.make_async_copy(view, view, sem).wait()

    def order_green():
        green_copy.wait()

        def one(g, carry):
            for j in range(chunks):
                for t in range(0, padded_x, 8):
                    tile = green_raw[g, j * kc:(j + 1) * kc, t:t + 8, :]
                    tile = jnp.swapaxes(tile, 0, 1)
                    for h in range(halves):
                        green[j, h, g, t:t + 8] = tile[:, :, h * 128:(h + 1) * 128]
            return carry

        lax.fori_loop(0, 6, one, 0)

    def middle(j):
        dims = (((1,), (0,)), ((), ()))
        for c in range(3):
            re = in_t[:, 2 * c, j * kc:(j + 1) * kc, :].reshape(cells_x * kc, cells_y)
            im = in_t[:, 2 * c + 1, j * kc:(j + 1) * kc, :].reshape(cells_x * kc, cells_y)
            pair = split(jnp.concatenate([re, im], axis=1))
            res = three_pass(pair, (wy_h[...], wy_l[...]), dims)
            for part in range(2):
                for h in range(halves):
                    at = part * padded_y + h * 128
                    spec[h, 2 * c + part] = res[:, at:at + 128].reshape(cells_x, kc, 128)

        def columns(h, carry):
            for c in range(3):
                line = [(spec[h, 2 * c, x], spec[h, 2 * c + 1, x]) for x in range(cells_x)]
                for m, (re, im) in enumerate(fft(line, -1)):
                    fld[2 * c, 2 * m], fld[2 * c + 1, 2 * m] = re, im
                line = [twiddle(*line[x], x, padded_x, -1) for x in range(cells_x)]
                for m, (re, im) in enumerate(fft(line, -1)):
                    fld[2 * c, 2 * m + 1], fld[2 * c + 1, 2 * m + 1] = re, im
            for kx in range(padded_x):
                g = [green[j, h, i, kx] for i in range(6)]
                for part in range(2):
                    s = [fld[2 * b + part, kx] for b in range(3)]
                    for a, row in enumerate(COMBOS):
                        fld[2 * a + part, kx] = g[row[0]] * s[0] + g[row[1]] * s[1] + g[row[2]] * s[2]
            for a in range(3):
                even = fft([(fld[2 * a, k], fld[2 * a + 1, k]) for k in range(0, padded_x, 2)], 1)
                for x in range(cells_x):
                    spec[h, 2 * a, x], spec[h, 2 * a + 1, x] = even[x]
                odd = fft([(fld[2 * a, k], fld[2 * a + 1, k]) for k in range(1, padded_x, 2)], 1)
                for x in range(cells_x):
                    re, im = twiddle(*odd[x], x, padded_x, 1)
                    spec[h, 2 * a, x] += re
                    spec[h, 2 * a + 1, x] += im
            return carry

        lax.fori_loop(0, halves, columns, 0)
        for a in range(3):
            parts = [
                spec[h, 2 * a + part].reshape(cells_x * kc, 128) for part in range(2) for h in range(halves)
            ]
            pair = split(jnp.concatenate(parts, axis=1))
            res = three_pass(pair, (vy_h[...], vy_l[...]), dims)
            for part in range(2):
                piece = res[:, part * cells_y:(part + 1) * cells_y].reshape(cells_x, kc, cells_y)
                out_u[:, 2 * a + part, j * kc:(j + 1) * kc, :] = piece

    for step in range(MATVECS):
        source, image = (pol_ref, first_ref) if step == 0 else (first_ref, second_ref)
        for c in range(3):
            forward_z(c, source[c, 0] * mask_ref[...])
        if step == 0:
            pl.semaphore_wait(barrier, n - 1)
        for j in range(chunks):
            exchange(out_t, in_t, j, fs_sem.at[step, j], fr_sem.at[step, j])
        if step == 0:
            order_green()
        for j in range(chunks):
            drain(in_t, fr_sem.at[step, j], j)
            middle(j)
            exchange(out_u, in_u, j, is_sem.at[step, j], ir_sem.at[step, j])
        for j in range(chunks):
            drain(out_t, fs_sem.at[step, j], j)
        for j in range(chunks):
            drain(in_u, ir_sem.at[step, j], j)
        for a in range(3):
            total = None
            for part in range(2):
                rows = slice(part * 2 * cells_z, (part + 1) * 2 * cells_z)
                field = in_u[:, 2 * a + part].reshape(2 * cells_z, cells_y)
                dims = (((0,), (0,)), ((), ()))
                term = three_pass(split(field), (vz_h[rows, :], vz_l[rows, :]), dims)
                total = term if total is None else total + term
            masked = source[a, 0] * mask_ref[...]
            image[a, 0] = inv_ref[0] * masked - mask_ref[...] * total
        for j in range(chunks):
            drain(out_u, is_sem.at[step, j], j)


def per_device(n, polarization, inverse_polarizability, occupancy, green_fourier):
    _, _, cells_y, cells_z = polarization.shape
    _, kz_own, padded_x, padded_y = green_fourier.shape
    padded_z = 2 * cells_z
    cells_x = padded_x // 2
    kc = min(8, kz_own)
    chunks = kz_own // kc
    halves = padded_y // 128
    cos, sin = tables(padded_z, cells_z, padded_z)
    wz = split_table(np.concatenate([cos, -sin], axis=0))
    cos, sin = tables(cells_y, padded_y, padded_y)
    wy = split_table(np.block([[cos, -sin], [sin, cos]]))
    cos, sin = tables(padded_y, cells_y, padded_y)
    vy = split_table(np.block([[cos, sin], [-sin, cos]]))
    cos, sin = tables(padded_z, cells_z, padded_z)
    vz = split_table(np.concatenate([cos, -sin], axis=0) / (padded_x * padded_y * padded_z))
    vmem = pl.BlockSpec(memory_space=pltpu.VMEM)
    sems = pltpu.SemaphoreType.DMA((MATVECS, chunks))
    return pl.pallas_call(
        functools.partial(kernel, n, cells_x, padded_x, kz_own, kc),
        out_shape=(jax.ShapeDtypeStruct(polarization.shape, F32),) * 2,
        in_specs=[vmem] * 3 + [pl.BlockSpec(memory_space=pl.ANY)] + [vmem] * 8,
        out_specs=(vmem, vmem),
        scratch_shapes=[
            pltpu.VMEM(green_fourier.shape, F32),
            pltpu.VMEM((chunks, halves, 6, padded_x, kc, 128), F32),
            pltpu.VMEM((cells_y, cells_z), F32),
            pltpu.VMEM((n, 6, kz_own, cells_y), F32),
            pltpu.VMEM((n, 6, kz_own, cells_y), F32),
            pltpu.VMEM((halves, 6, cells_x, kc, 128), F32),
            pltpu.VMEM((6, padded_x, kc, 128), F32),
            pltpu.VMEM((n, 6, kz_own, cells_y), F32),
            pltpu.VMEM((n, 6, kz_own, cells_y), F32),
            pltpu.SemaphoreType.DMA,
            sems, sems, sems, sems,
        ],
        compiler_params=pltpu.CompilerParams(
            collective_id=0, has_side_effects=True, vmem_limit_bytes=60 * 1024 * 1024
        ),
    )(polarization, inverse_polarizability, occupancy, green_fourier, *map(jnp.asarray, wz + wy + vy + vz))


def solution(mesh):
    return jax.shard_map(
        functools.partial(per_device, mesh.shape["slab"]),
        mesh=mesh,
        in_specs=(
            P("comp", "slab", None, None),
            P("slab", None, None),
            P("slab", None, None),
            P(None, "slab", None, None),
        ),
        out_specs=(P("comp", "slab", None, None), P("comp", "slab", None, None)),
        check_vma=False,
    )
```

```python
import functools
import math

import jax
import jax.numpy as jnp
import numpy as np
from jax import lax
from jax.experimental import pallas as pl
from jax.experimental.pallas import tpu as pltpu
from jax.sharding import PartitionSpec as P

BLOCK = 8
MATVECS = 2
F32 = jnp.float32
BF16 = jnp.bfloat16
COMBOS = ((0, 3, 4), (3, 1, 5), (4, 5, 2))


def tables(count_in, count_out, length):
    phase = np.arange(count_in)[:, None] * np.arange(count_out)[None, :] % length
    angle = phase * (2.0 * math.pi / length)
    return np.cos(angle), np.sin(angle)


def split_table(table):
    table = table.astype(np.float32)
    high = table.astype(jnp.bfloat16)
    low = (table - high.astype(np.float32)).astype(jnp.bfloat16)
    return high, low


def split(value):
    high = value.astype(BF16)
    return high, (value - high.astype(F32)).astype(BF16)


def twiddle(re, im, num, length, sign):
    num = num * sign % length
    if num == 0:
        return re, im
    if 4 * num == length:
        return -im, re
    if 2 * num == length:
        return -re, -im
    if 4 * num == 3 * length:
        return im, -re
    c = math.cos(2.0 * math.pi * num / length)
    s = math.sin(2.0 * math.pi * num / length)
    if (8 * num) % length == 0:
        a = abs(c)
        p, m = (re + im) * a, (re - im) * a
        return {1: (m, p), 3: (-p, m), 5: (-m, -p), 7: (p, -m)}[8 * num // length]
    return re * c - im * s, re * s + im * c


def fft(values, sign):
    n = len(values)
    if n == 1:
        return values
    even, odd = fft(values[0::2], sign), fft(values[1::2], sign)
    low, high = [], []
    for k in range(n // 2):
        (er, ei), (o_r, oi) = even[k], twiddle(*odd[k], k, n, sign)
        low.append((er + o_r, ei + oi))
        high.append((er - o_r, ei - oi))
    return low + high


def three_pass(pair, table_pair, dims):
    dot = functools.partial(lax.dot_general, dimension_numbers=dims, preferred_element_type=F32)
    (vh, vl), (th, tl) = pair, table_pair
    return dot(vh, th) + (dot(vl, th) + dot(vh, tl))


def kernel(
    n, cells_x, padded_x, kz_own, kc,
    pol_ref, inv_ref, occ_ref, green_ref, wz_h, wz_l, wy_h, wy_l, vy_h, vy_l, vz_h, vz_l,
    first_ref, second_ref,
    green_raw, green, mask_ref, raw_out, raw_in, out_t, in_t, lines, spec, out_u, in_u, part_out, part_in,
    green_sem, ws_sem, wr_sem, ts_sem, tr_sem, cs_sem, cr_sem, os_sem, or_sem, ps_sem, pr_sem,
):
    me = lax.axis_index("slab")
    group = n // 2
    here = me // group
    seat = lax.rem(me, group)
    twin = lax.rem(me + group, n)
    base = here * group
    chunks = kz_own // kc
    cells_y, cells_z = mask_ref.shape
    padded_y = 2 * cells_y
    halves = padded_y // 128
    kz_half = group * kz_own
    green_copy = pltpu.make_async_copy(green_ref, green_raw, green_sem)
    green_copy.start()

    def signal(device):
        pl.semaphore_signal(barrier, inc=1, device_id={"slab": device}, device_id_type=pl.DeviceIdType.MESH)

    def remote(source, target, send_sem, recv_sem, device):
        return pltpu.make_async_remote_copy(
            src_ref=source, dst_ref=target, send_sem=send_sem, recv_sem=recv_sem,
            device_id={"slab": device}, device_id_type=pl.DeviceIdType.MESH,
        )

    barrier = pltpu.get_barrier_semaphore()
    signal(twin)

    def greet(k, carry):
        signal(base + lax.rem(seat + k, group))
        return carry

    lax.fori_loop(1, group, greet, 0)

    blocks_y, blocks_z = occ_ref.shape[1:]
    up_y = lax.broadcasted_iota(jnp.int32, (cells_y, blocks_y), 0) // BLOCK
    up_y = (up_y == lax.broadcasted_iota(jnp.int32, (cells_y, blocks_y), 1)).astype(F32).astype(BF16)
    up_z = lax.broadcasted_iota(jnp.int32, (blocks_z, cells_z), 1) // BLOCK
    up_z = (up_z == lax.broadcasted_iota(jnp.int32, (blocks_z, cells_z), 0)).astype(F32).astype(BF16)
    flags = occ_ref[0].astype(F32).astype(BF16)
    spread = jnp.dot(up_y, flags, preferred_element_type=F32).astype(BF16)
    mask_ref[...] = jnp.dot(spread, up_z, preferred_element_type=F32)

    def order_green():
        green_copy.wait()

        def one(g, carry):
            for j in range(chunks):
                for t in range(0, padded_x, 8):
                    tile = green_raw[g, j * kc:(j + 1) * kc, t:t + 8, :]
                    tile = jnp.swapaxes(tile, 0, 1)
                    for h in range(halves):
                        green[j * halves + h, g, t:t + 8] = tile[:, :, h * 128:(h + 1) * 128]
            return carry

        lax.fori_loop(0, 6, one, 0)

    def send_raw(step, c, field):
        raw_out[c] = field
        remote(raw_out.at[c], raw_in.at[c], ws_sem.at[step, c], wr_sem.at[step, c], twin).start()

    def forward_z(step, c, which, field):
        pair = split(field)
        slab = me if which == 0 else twin
        for part in range(2):
            dims = (((1,), (1,)), ((), ()))
            res = three_pass((wz_h[here, part], wz_l[here, part]), pair, dims)
            out_t[c, which, :, part] = res.reshape(group, kz_own, cells_y)

        def send(k, carry):
            to = lax.rem(seat + k, group)
            remote(
                out_t.at[c, which, to], in_t.at[c, slab], ts_sem.at[step, c], tr_sem.at[step, c], base + to
            ).start()
            return carry

        lax.fori_loop(1, group, send, 0)
        in_t[c, slab] = out_t[c, which, seat]

    def drain(view, sem):
        pltpu.make_async_copy(view, view, sem).wait()

    def forward_yx(step, c):
        drain(in_t.at[c, pl.ds(0, n - 2)], tr_sem.at[step, c])
        parts = [in_t[c, :, part].reshape(cells_x * kz_own, cells_y) for part in range(2)]
        dims = (((1,), (0,)), ((), ()))
        res = three_pass(split(jnp.concatenate(parts, axis=1)), (wy_h[...], wy_l[...]), dims)
        for part in range(2):
            for h in range(halves):
                at = part * padded_y + h * 128
                piece = res[:, at:at + 128].reshape(cells_x, kz_own, 128)
                for j in range(chunks):
                    lines[j * halves + h, part] = piece[:, j * kc:(j + 1) * kc]

        def columns(i, carry):
            line = [(lines[i, 0, x], lines[i, 1, x]) for x in range(cells_x)]
            for m, (re, im) in enumerate(fft(line, -1)):
                spec[i, 2 * c, 2 * m], spec[i, 2 * c + 1, 2 * m] = re, im
            line = [twiddle(lines[i, 0, x], lines[i, 1, x], x, padded_x, -1) for x in range(cells_x)]
            for m, (re, im) in enumerate(fft(line, -1)):
                spec[i, 2 * c, 2 * m + 1], spec[i, 2 * c + 1, 2 * m + 1] = re, im
            return carry

        lax.fori_loop(0, chunks * halves, columns, 0)

    def backward_xy(step, a):
        row = COMBOS[a]

        def columns(i, carry):
            def field(k):
                g = [green[i, r, k] for r in row]
                s = [spec[i, r, k] for r in range(6)]
                return g[0] * s[0] + g[1] * s[2] + g[2] * s[4], g[0] * s[1] + g[1] * s[3] + g[2] * s[5]

            even = fft([field(k) for k in range(0, padded_x, 2)], 1)
            for x in range(cells_x):
                lines[i, 0, x], lines[i, 1, x] = even[x]
            odd = fft([field(k) for k in range(1, padded_x, 2)], 1)
            for x in range(cells_x):
                re, im = twiddle(*odd[x], x, padded_x, 1)
                lines[i, 0, x] += re
                lines[i, 1, x] += im
            return carry

        lax.fori_loop(0, chunks * halves, columns, 0)
        parts = []
        for part in range(2):
            for h in range(halves):
                pieces = [lines[j * halves + h, part] for j in range(chunks)]
                piece = pieces[0] if chunks == 1 else jnp.concatenate(pieces, axis=1)
                parts.append(piece.reshape(cells_x * kz_own, 128))
        dims = (((1,), (0,)), ((), ()))
        res = three_pass(split(jnp.concatenate(parts, axis=1)), (vy_h[...], vy_l[...]), dims)
        for part in range(2):
            piece = res[:, part * cells_y:(part + 1) * cells_y]
            out_u[a, :, part] = piece.reshape(cells_x, kz_own, cells_y)
        there = (1 - here) * group
        for which, first, s_sem, r_sem in ((1, there, cs_sem, cr_sem), (0, base, os_sem, or_sem)):

            def send(k, carry):
                to = lax.rem(seat + k, group)
                remote(
                    out_u.at[a, first + to], in_u.at[a, which, seat], s_sem.at[step, a], r_sem.at[step, a], base + to
                ).start()
                return carry

            lax.fori_loop(1, group, send, 0)
            in_u[a, which, seat] = out_u[a, first + seat]

    def inverse_z(a, which):
        total = None
        for part in range(2):
            field = in_u[a, which, :, part].reshape(kz_half, cells_y)
            dims = (((0,), (0,)), ((), ()))
            term = three_pass(split(field), (vz_h[here, part], vz_l[here, part]), dims)
            total = term if total is None else total + term
        return total

    def send_part(step, a):
        drain(in_u.at[a, 1, pl.ds(0, group - 1)], cr_sem.at[step, a])
        part_out[a] = inverse_z(a, 1)
        remote(part_out.at[a], part_in.at[a], ps_sem.at[step, a], pr_sem.at[step, a], twin).start()

    for step in range(MATVECS):
        source, image = (pol_ref, first_ref) if step == 0 else (first_ref, second_ref)
        if step == 0:
            pl.semaphore_wait(barrier, group)
            for c in range(3):
                send_raw(step, c, source[c, 0] * mask_ref[...])
            for c in range(3):
                forward_z(step, c, 0, raw_out[c])
            order_green()
        for c in range(3):
            drain(raw_in.at[c], wr_sem.at[step, c])
            forward_z(step, c, 1, raw_in[c])
            if c > 0:
                forward_yx(step, c - 1)
        forward_yx(step, 2)
        for a in range(3):
            backward_xy(step, a)
            if a > 0:
                send_part(step, a - 1)
        send_part(step, 2)
        for c in range(3):
            drain(raw_out.at[c], ws_sem.at[step, c])
            drain(in_t.at[c, pl.ds(0, n - 2)], ts_sem.at[step, c])
        for a in range(3):
            drain(in_u.at[a, 0, pl.ds(0, group - 1)], or_sem.at[step, a])
            own = inverse_z(a, 0)
            masked = source[a, 0] * mask_ref[...]
            drain(part_in.at[a], pr_sem.at[step, a])
            image[a, 0] = inv_ref[0] * masked - mask_ref[...] * (own + part_in[a])
            if step + 1 < MATVECS:
                send_raw(step + 1, a, image[a, 0] * mask_ref[...])
                forward_z(step + 1, a, 0, raw_out[a])
        for a in range(3):
            drain(in_u.at[a, 1, pl.ds(0, group - 1)], cs_sem.at[step, a])
            drain(in_u.at[a, 0, pl.ds(0, group - 1)], os_sem.at[step, a])
            drain(part_out.at[a], ps_sem.at[step, a])


def per_device(n, polarization, inverse_polarizability, occupancy, green_fourier):
    _, _, cells_y, cells_z = polarization.shape
    _, kz_own, padded_x, padded_y = green_fourier.shape
    padded_z = 2 * cells_z
    cells_x = padded_x // 2
    kc = min(8, kz_own)
    chunks = kz_own // kc
    halves = padded_y // 128
    cos, sin = tables(padded_z, cells_z, padded_z)
    wz = split_table(np.stack([cos, -sin]).reshape(2, 2, cells_z, cells_z).swapaxes(0, 1))
    cos, sin = tables(cells_y, padded_y, padded_y)
    wy = split_table(np.block([[cos, -sin], [sin, cos]]))
    cos, sin = tables(padded_y, cells_y, padded_y)
    vy = split_table(np.block([[cos, sin], [-sin, cos]]))
    cos, sin = tables(padded_z, cells_z, padded_z)
    vz = np.stack([cos, -sin]).reshape(2, 2, cells_z, cells_z).swapaxes(0, 1)
    vz = split_table(vz / (padded_x * padded_y * padded_z))
    vmem = pl.BlockSpec(memory_space=pltpu.VMEM)
    return pl.pallas_call(
        functools.partial(kernel, n, cells_x, padded_x, kz_own, kc),
        out_shape=(jax.ShapeDtypeStruct(polarization.shape, F32),) * 2,
        in_specs=[vmem] * 3 + [pl.BlockSpec(memory_space=pl.ANY)] + [vmem] * 8,
        out_specs=(vmem, vmem),
        scratch_shapes=[
            pltpu.VMEM(green_fourier.shape, F32),
            pltpu.VMEM((chunks * halves, 6, padded_x, kc, 128), F32),
            pltpu.VMEM((cells_y, cells_z), F32),
            pltpu.VMEM((3, cells_y, cells_z), F32),
            pltpu.VMEM((3, cells_y, cells_z), F32),
            pltpu.VMEM((3, 2, n // 2, 2, kz_own, cells_y), F32),
            pltpu.VMEM((3, n, 2, kz_own, cells_y), F32),
            pltpu.VMEM((chunks * halves, 2, cells_x, kc, 128), F32),
            pltpu.VMEM((chunks * halves, 6, padded_x, kc, 128), F32),
            pltpu.VMEM((3, n, 2, kz_own, cells_y), F32),
            pltpu.VMEM((3, 2, n // 2, 2, kz_own, cells_y), F32),
            pltpu.VMEM((3, cells_y, cells_z), F32),
            pltpu.VMEM((3, cells_y, cells_z), F32),
            pltpu.SemaphoreType.DMA,
            *[pltpu.SemaphoreType.DMA((MATVECS, 3))] * 10,
        ],
        compiler_params=pltpu.CompilerParams(
            collective_id=0, has_side_effects=True, vmem_limit_bytes=60 * 1024 * 1024
        ),
    )(polarization, inverse_polarizability, occupancy, green_fourier, *map(jnp.asarray, wz + wy + vy + vz))


def solution(mesh):
    return jax.shard_map(
        functools.partial(per_device, mesh.shape["slab"]),
        mesh=mesh,
        in_specs=(
            P("comp", "slab", None, None),
            P("slab", None, None),
            P("slab", None, None),
            P(None, "slab", None, None),
        ),
        out_specs=(P("comp", "slab", None, None), P("comp", "slab", None, None)),
        check_vma=False,
    )
```

```python
import functools
import math

import jax
import jax.numpy as jnp
import numpy as np
from jax import lax
from jax.experimental import pallas as pl
from jax.experimental.pallas import tpu as pltpu
from jax.sharding import PartitionSpec as P

BLOCK = 8
MATVECS = 2
F32 = jnp.float32
BF16 = jnp.bfloat16
COMBOS = ((0, 3, 4), (3, 1, 5), (4, 5, 2))


def tables(count_in, count_out, length):
    phase = np.arange(count_in)[:, None] * np.arange(count_out)[None, :] % length
    angle = phase * (2.0 * math.pi / length)
    return np.cos(angle), np.sin(angle)


def split_table(table):
    table = table.astype(np.float32)
    high = table.astype(jnp.bfloat16)
    low = (table - high.astype(np.float32)).astype(jnp.bfloat16)
    return high, low


def split(value):
    high = value.astype(BF16)
    return high, (value - high.astype(F32)).astype(BF16)


def twiddle(re, im, num, length, sign):
    num = num * sign % length
    if num == 0:
        return re, im
    if 4 * num == length:
        return -im, re
    if 2 * num == length:
        return -re, -im
    if 4 * num == 3 * length:
        return im, -re
    c = math.cos(2.0 * math.pi * num / length)
    s = math.sin(2.0 * math.pi * num / length)
    if (8 * num) % length == 0:
        a = abs(c)
        p, m = (re + im) * a, (re - im) * a
        return {1: (m, p), 3: (-p, m), 5: (-m, -p), 7: (p, -m)}[8 * num // length]
    return re * c - im * s, re * s + im * c


def fft(values, sign):
    n = len(values)
    if n == 1:
        return values
    even, odd = fft(values[0::2], sign), fft(values[1::2], sign)
    low, high = [], []
    for k in range(n // 2):
        (er, ei), (o_r, oi) = even[k], twiddle(*odd[k], k, n, sign)
        low.append((er + o_r, ei + oi))
        high.append((er - o_r, ei - oi))
    return low + high


def three_pass(pair, table_pair, dims):
    dot = functools.partial(lax.dot_general, dimension_numbers=dims, preferred_element_type=F32)
    (vh, vl), (th, tl) = pair, table_pair
    return dot(vh, th) + (dot(vl, th) + dot(vh, tl))


def kernel(
    n, cells_x, padded_x, kz_own, kc,
    pol_ref, inv_ref, occ_ref, green_ref, wz_h, wz_l, wy_h, wy_l, vy_h, vy_l, vz_h, vz_l,
    first_ref, second_ref,
    green_raw, green, mask_ref, raw_out, raw_in, out_t, in_t, lines, spec, out_u, in_u, part_out, part_in,
    green_sem, ws_sem, wr_sem, ts_sem, tr_sem, cs_sem, cr_sem, os_sem, or_sem, ps_sem, pr_sem,
):
    me = lax.axis_index("slab")
    group = n // 2
    here = me // group
    seat = lax.rem(me, group)
    twin = lax.rem(me + group, n)
    base = here * group
    chunks = kz_own // kc
    cells_y, cells_z = mask_ref.shape
    padded_y = 2 * cells_y
    halves = padded_y // 128
    kz_half = group * kz_own
    green_copy = pltpu.make_async_copy(green_ref, green_raw, green_sem)
    green_copy.start()

    def signal(device):
        pl.semaphore_signal(barrier, inc=1, device_id={"slab": device}, device_id_type=pl.DeviceIdType.MESH)

    def remote(source, target, send_sem, recv_sem, device):
        return pltpu.make_async_remote_copy(
            src_ref=source, dst_ref=target, send_sem=send_sem, recv_sem=recv_sem,
            device_id={"slab": device}, device_id_type=pl.DeviceIdType.MESH,
        )

    barrier = pltpu.get_barrier_semaphore()
    signal(twin)

    def greet(k, carry):
        signal(base + lax.rem(seat + k, group))
        return carry

    lax.fori_loop(1, group, greet, 0)

    blocks_y, blocks_z = occ_ref.shape[1:]
    up_y = lax.broadcasted_iota(jnp.int32, (cells_y, blocks_y), 0) // BLOCK
    up_y = (up_y == lax.broadcasted_iota(jnp.int32, (cells_y, blocks_y), 1)).astype(F32).astype(BF16)
    up_z = lax.broadcasted_iota(jnp.int32, (blocks_z, cells_z), 1) // BLOCK
    up_z = (up_z == lax.broadcasted_iota(jnp.int32, (blocks_z, cells_z), 0)).astype(F32).astype(BF16)
    flags = occ_ref[0].astype(F32).astype(BF16)
    spread = jnp.dot(up_y, flags, preferred_element_type=F32).astype(BF16)
    mask_ref[...] = jnp.dot(spread, up_z, preferred_element_type=F32)

    def order_green():
        green_copy.wait()

        def one(g, carry):
            for j in range(chunks):
                for t in range(0, padded_x, 8):
                    tile = green_raw[g, j * kc:(j + 1) * kc, t:t + 8, :]
                    tile = jnp.swapaxes(tile, 0, 1)
                    for h in range(halves):
                        green[j * halves + h, g, t:t + 8] = tile[:, :, h * 128:(h + 1) * 128]
            return carry

        lax.fori_loop(0, 6, one, 0)

    def send_raw(step, c, field):
        raw_out[c] = field
        remote(raw_out.at[c], raw_in.at[c], ws_sem.at[step, c], wr_sem.at[step, c], twin).start()

    def forward_z(step, c, which, field):
        pair = split(field)
        slab = me if which == 0 else twin
        for part in range(2):
            dims = (((1,), (1,)), ((), ()))
            res = three_pass((wz_h[here, part], wz_l[here, part]), pair, dims)
            out_t[c, which, :, part] = res.reshape(group, kz_own, cells_y)

        def send(k, carry):
            to = lax.rem(seat + k, group)
            remote(
                out_t.at[c, which, to], in_t.at[c, slab], ts_sem.at[step, c], tr_sem.at[step, c], base + to
            ).start()
            return carry

        lax.fori_loop(1, group, send, 0)
        in_t[c, slab] = out_t[c, which, seat]

    def drain(view, sem):
        pltpu.make_async_copy(view, view, sem).wait()

    def forward_yx(step, c):
        drain(in_t.at[c, pl.ds(0, n - 2)], tr_sem.at[step, c])
        parts = [in_t[c, :, part].reshape(cells_x * kz_own, cells_y) for part in range(2)]
        dims = (((1,), (0,)), ((), ()))
        res = three_pass(split(jnp.concatenate(parts, axis=1)), (wy_h[...], wy_l[...]), dims)
        for part in range(2):
            for h in range(halves):
                at = part * padded_y + h * 128
                piece = res[:, at:at + 128].reshape(cells_x, kz_own, 128)
                for j in range(chunks):
                    lines[j * halves + h, part] = piece[:, j * kc:(j + 1) * kc]

        def columns(i, carry):
            line = [(lines[i, 0, x], lines[i, 1, x]) for x in range(cells_x)]
            for m, (re, im) in enumerate(fft(line, -1)):
                spec[i, 2 * c, 2 * m], spec[i, 2 * c + 1, 2 * m] = re, im
            line = [twiddle(lines[i, 0, x], lines[i, 1, x], x, padded_x, -1) for x in range(cells_x)]
            for m, (re, im) in enumerate(fft(line, -1)):
                spec[i, 2 * c, 2 * m + 1], spec[i, 2 * c + 1, 2 * m + 1] = re, im
            return carry

        lax.fori_loop(0, chunks * halves, columns, 0)

    def backward_xy(step, a):
        row = COMBOS[a]

        def columns(i, carry):
            def field(k):
                g = [green[i, r, k] for r in row]
                s = [spec[i, r, k] for r in range(6)]
                return g[0] * s[0] + g[1] * s[2] + g[2] * s[4], g[0] * s[1] + g[1] * s[3] + g[2] * s[5]

            even = fft([field(k) for k in range(0, padded_x, 2)], 1)
            for x in range(cells_x):
                lines[i, 0, x], lines[i, 1, x] = even[x]
            odd = fft([field(k) for k in range(1, padded_x, 2)], 1)
            for x in range(cells_x):
                re, im = twiddle(*odd[x], x, padded_x, 1)
                lines[i, 0, x] += re
                lines[i, 1, x] += im
            return carry

        lax.fori_loop(0, chunks * halves, columns, 0)
        parts = []
        for part in range(2):
            for h in range(halves):
                pieces = [lines[j * halves + h, part] for j in range(chunks)]
                piece = pieces[0] if chunks == 1 else jnp.concatenate(pieces, axis=1)
                parts.append(piece.reshape(cells_x * kz_own, 128))
        dims = (((1,), (0,)), ((), ()))
        res = three_pass(split(jnp.concatenate(parts, axis=1)), (vy_h[...], vy_l[...]), dims)
        for part in range(2):
            piece = res[:, part * cells_y:(part + 1) * cells_y]
            out_u[a, :, part] = piece.reshape(cells_x, kz_own, cells_y)
        send_back(step, a, 1, (1 - here) * group, cs_sem, cr_sem)

    def send_back(step, a, which, first, s_sem, r_sem):
        def send(k, carry):
            to = lax.rem(seat + k, group)
            remote(
                out_u.at[a, first + to], in_u.at[a, which, seat], s_sem.at[step, a], r_sem.at[step, a], base + to
            ).start()
            return carry

        lax.fori_loop(1, group, send, 0)
        in_u[a, which, seat] = out_u[a, first + seat]

    def inverse_z(a, which):
        total = None
        for part in range(2):
            field = in_u[a, which, :, part].reshape(kz_half, cells_y)
            dims = (((0,), (0,)), ((), ()))
            term = three_pass(split(field), (vz_h[here, part], vz_l[here, part]), dims)
            total = term if total is None else total + term
        return total

    def send_part(step, a):
        drain(in_u.at[a, 1, pl.ds(0, group - 1)], cr_sem.at[step, a])
        part_out[a] = inverse_z(a, 1)
        remote(part_out.at[a], part_in.at[a], ps_sem.at[step, a], pr_sem.at[step, a], twin).start()

    for step in range(MATVECS):
        source, image = (pol_ref, first_ref) if step == 0 else (first_ref, second_ref)
        if step == 0:
            pl.semaphore_wait(barrier, group)
            for c in range(3):
                send_raw(step, c, source[c, 0] * mask_ref[...])
            for c in range(3):
                forward_z(step, c, 0, raw_out[c])
            order_green()
        for c in range(3):
            drain(raw_in.at[c], wr_sem.at[step, c])
            forward_z(step, c, 1, raw_in[c])
            if c > 0:
                forward_yx(step, c - 1)
        forward_yx(step, 2)
        for a in range(3):
            backward_xy(step, a)
            if a == 1:
                send_part(step, 0)
        for a in range(3):
            send_back(step, a, 0, base, os_sem, or_sem)
        send_part(step, 1)
        send_part(step, 2)
        for c in range(3):
            drain(raw_out.at[c], ws_sem.at[step, c])
            drain(in_t.at[c, pl.ds(0, n - 2)], ts_sem.at[step, c])
        for a in range(3):
            drain(in_u.at[a, 0, pl.ds(0, group - 1)], or_sem.at[step, a])
            own = inverse_z(a, 0)
            masked = source[a, 0] * mask_ref[...]
            drain(part_in.at[a], pr_sem.at[step, a])
            image[a, 0] = inv_ref[0] * masked - mask_ref[...] * (own + part_in[a])
            if step + 1 < MATVECS:
                send_raw(step + 1, a, image[a, 0] * mask_ref[...])
                forward_z(step + 1, a, 0, raw_out[a])
        for a in range(3):
            drain(in_u.at[a, 1, pl.ds(0, group - 1)], cs_sem.at[step, a])
            drain(in_u.at[a, 0, pl.ds(0, group - 1)], os_sem.at[step, a])
            drain(part_out.at[a], ps_sem.at[step, a])


def deliver(first_ref, second_ref, first_out, second_out, first, second, in_sem, out_sem):
    loads = [
        pltpu.make_async_copy(source, held, in_sem.at[i])
        for i, (source, held) in enumerate(((first_ref, first), (second_ref, second)))
    ]
    stores = [
        pltpu.make_async_copy(held, target, out_sem.at[i])
        for i, (held, target) in enumerate(((first, first_out), (second, second_out)))
    ]
    for copy in loads:
        copy.start()
    for load, store in zip(loads, stores):
        load.wait()
        store.start()
    for store in stores:
        store.wait()


def per_device(n, polarization, inverse_polarizability, occupancy, green_fourier):
    _, _, cells_y, cells_z = polarization.shape
    _, kz_own, padded_x, padded_y = green_fourier.shape
    padded_z = 2 * cells_z
    cells_x = padded_x // 2
    kc = min(8, kz_own)
    chunks = kz_own // kc
    halves = padded_y // 128
    cos, sin = tables(padded_z, cells_z, padded_z)
    wz = split_table(np.stack([cos, -sin]).reshape(2, 2, cells_z, cells_z).swapaxes(0, 1))
    cos, sin = tables(cells_y, padded_y, padded_y)
    wy = split_table(np.block([[cos, -sin], [sin, cos]]))
    cos, sin = tables(padded_y, cells_y, padded_y)
    vy = split_table(np.block([[cos, sin], [-sin, cos]]))
    cos, sin = tables(padded_z, cells_z, padded_z)
    vz = np.stack([cos, -sin]).reshape(2, 2, cells_z, cells_z).swapaxes(0, 1)
    vz = split_table(vz / (padded_x * padded_y * padded_z))
    vmem = pl.BlockSpec(memory_space=pltpu.VMEM)
    images = pl.pallas_call(
        functools.partial(kernel, n, cells_x, padded_x, kz_own, kc),
        out_shape=(jax.ShapeDtypeStruct(polarization.shape, F32),) * 2,
        in_specs=[vmem] * 3 + [pl.BlockSpec(memory_space=pl.ANY)] + [vmem] * 8,
        out_specs=(vmem, vmem),
        scratch_shapes=[
            pltpu.VMEM(green_fourier.shape, F32),
            pltpu.VMEM((chunks * halves, 6, padded_x, kc, 128), F32),
            pltpu.VMEM((cells_y, cells_z), F32),
            pltpu.VMEM((3, cells_y, cells_z), F32),
            pltpu.VMEM((3, cells_y, cells_z), F32),
            pltpu.VMEM((3, 2, n // 2, 2, kz_own, cells_y), F32),
            pltpu.VMEM((3, n, 2, kz_own, cells_y), F32),
            pltpu.VMEM((chunks * halves, 2, cells_x, kc, 128), F32),
            pltpu.VMEM((chunks * halves, 6, padded_x, kc, 128), F32),
            pltpu.VMEM((3, n, 2, kz_own, cells_y), F32),
            pltpu.VMEM((3, 2, n // 2, 2, kz_own, cells_y), F32),
            pltpu.VMEM((3, cells_y, cells_z), F32),
            pltpu.VMEM((3, cells_y, cells_z), F32),
            pltpu.SemaphoreType.DMA,
            *[pltpu.SemaphoreType.DMA((MATVECS, 3))] * 10,
        ],
        compiler_params=pltpu.CompilerParams(
            collective_id=0, has_side_effects=True, vmem_limit_bytes=60 * 1024 * 1024
        ),
    )(polarization, inverse_polarizability, occupancy, green_fourier, *map(jnp.asarray, wz + wy + vy + vz))
    anywhere = pl.BlockSpec(memory_space=pl.ANY)
    return pl.pallas_call(
        deliver,
        out_shape=(jax.ShapeDtypeStruct(polarization.shape, F32),) * 2,
        in_specs=[anywhere] * 2,
        out_specs=(anywhere, anywhere),
        scratch_shapes=[pltpu.VMEM(polarization.shape, F32)] * 2 + [pltpu.SemaphoreType.DMA((2,))] * 2,
    )(*images)


def solution(mesh):
    return jax.shard_map(
        functools.partial(per_device, mesh.shape["slab"]),
        mesh=mesh,
        in_specs=(
            P("comp", "slab", None, None),
            P("slab", None, None),
            P("slab", None, None),
            P(None, "slab", None, None),
        ),
        out_specs=(P("comp", "slab", None, None), P("comp", "slab", None, None)),
        check_vma=False,
    )
```

```python
import functools
import math

import jax
import jax.numpy as jnp
import numpy as np
from jax import lax
from jax.experimental import pallas as pl
from jax.experimental.pallas import tpu as pltpu
from jax.sharding import PartitionSpec as P

BLOCK = 8
MATVECS = 2
F32 = jnp.float32
BF16 = jnp.bfloat16
COMBOS = ((0, 3, 4), (3, 1, 5), (4, 5, 2))


def tables(count_in, count_out, length):
    phase = np.arange(count_in)[:, None] * np.arange(count_out)[None, :] % length
    angle = phase * (2.0 * math.pi / length)
    return np.cos(angle), np.sin(angle)


def split_table(table):
    table = table.astype(np.float32)
    high = table.astype(jnp.bfloat16)
    low = (table - high.astype(np.float32)).astype(jnp.bfloat16)
    return high, low


def split(value):
    high = value.astype(BF16)
    return high, (value - high.astype(F32)).astype(BF16)


def twiddle(re, im, num, length, sign):
    num = num * sign % length
    if num == 0:
        return re, im
    if 4 * num == length:
        return -im, re
    if 2 * num == length:
        return -re, -im
    if 4 * num == 3 * length:
        return im, -re
    c = math.cos(2.0 * math.pi * num / length)
    s = math.sin(2.0 * math.pi * num / length)
    if (8 * num) % length == 0:
        a = abs(c)
        p, m = (re + im) * a, (re - im) * a
        return {1: (m, p), 3: (-p, m), 5: (-m, -p), 7: (p, -m)}[8 * num // length]
    return re * c - im * s, re * s + im * c


def fft(values, sign):
    n = len(values)
    if n == 1:
        return values
    even, odd = fft(values[0::2], sign), fft(values[1::2], sign)
    low, high = [], []
    for k in range(n // 2):
        (er, ei), (o_r, oi) = even[k], twiddle(*odd[k], k, n, sign)
        low.append((er + o_r, ei + oi))
        high.append((er - o_r, ei - oi))
    return low + high


def three_pass(pair, table_pair, dims):
    dot = functools.partial(lax.dot_general, dimension_numbers=dims, preferred_element_type=F32)
    (vh, vl), (th, tl) = pair, table_pair
    return dot(vh, th) + (dot(vl, th) + dot(vh, tl))


def kernel(
    n, cells_x, padded_x, kz_own, kc,
    pol_ref, inv_ref, occ_ref, green_ref, wz_h, wz_l, wy_h, wy_l, vy_h, vy_l, vz_h, vz_l,
    first_ref, second_ref,
    green_raw, green, mask_ref, raw_out, raw_in, out_t, in_t, lines, spec, out_u, in_u, part_out, part_in,
    green_sem, ws_sem, wr_sem, ts_sem, tr_sem, cs_sem, cr_sem, os_sem, or_sem, ps_sem, pr_sem,
):
    me = lax.axis_index("slab")
    group = n // 2
    here = me // group
    seat = lax.rem(me, group)
    twin = lax.rem(me + group, n)
    base = here * group
    chunks = kz_own // kc
    cells_y, cells_z = mask_ref.shape
    padded_y = 2 * cells_y
    halves = padded_y // 128
    kz_half = group * kz_own
    green_copy = pltpu.make_async_copy(green_ref, green_raw, green_sem)
    green_copy.start()

    def signal(device):
        pl.semaphore_signal(barrier, inc=1, device_id={"slab": device}, device_id_type=pl.DeviceIdType.MESH)

    def remote(source, target, send_sem, recv_sem, device):
        return pltpu.make_async_remote_copy(
            src_ref=source, dst_ref=target, send_sem=send_sem, recv_sem=recv_sem,
            device_id={"slab": device}, device_id_type=pl.DeviceIdType.MESH,
        )

    barrier = pltpu.get_barrier_semaphore()
    signal(twin)

    def greet(k, carry):
        signal(base + lax.rem(seat + k, group))
        return carry

    lax.fori_loop(1, group, greet, 0)

    blocks_y, blocks_z = occ_ref.shape[1:]
    up_y = lax.broadcasted_iota(jnp.int32, (cells_y, blocks_y), 0) // BLOCK
    up_y = (up_y == lax.broadcasted_iota(jnp.int32, (cells_y, blocks_y), 1)).astype(F32).astype(BF16)
    up_z = lax.broadcasted_iota(jnp.int32, (blocks_z, cells_z), 1) // BLOCK
    up_z = (up_z == lax.broadcasted_iota(jnp.int32, (blocks_z, cells_z), 0)).astype(F32).astype(BF16)
    flags = occ_ref[0].astype(F32).astype(BF16)
    spread = jnp.dot(up_y, flags, preferred_element_type=F32).astype(BF16)
    mask_ref[...] = jnp.dot(spread, up_z, preferred_element_type=F32)

    def order_green():
        green_copy.wait()

        def one(g, carry):
            for j in range(chunks):
                for t in range(0, padded_x, 8):
                    tile = green_raw[g, j * kc:(j + 1) * kc, t:t + 8, :]
                    tile = jnp.swapaxes(tile, 0, 1)
                    for h in range(halves):
                        green[j * halves + h, g, t:t + 8] = tile[:, :, h * 128:(h + 1) * 128]
            return carry

        lax.fori_loop(0, 6, one, 0)

    def send_raw(step, c, field):
        raw_out[c] = field
        remote(raw_out.at[c], raw_in.at[c], ws_sem.at[step, c], wr_sem.at[step, c], twin).start()

    def forward_z(step, c, which, field):
        pair = split(field)
        slab = me if which == 0 else twin
        for part in range(2):
            dims = (((1,), (1,)), ((), ()))
            res = three_pass((wz_h[here, part], wz_l[here, part]), pair, dims)
            out_t[c, which, :, part] = res.reshape(group, kz_own, cells_y)

        def send(k, carry):
            to = lax.rem(seat + k, group)
            remote(
                out_t.at[c, which, to], in_t.at[c, slab], ts_sem.at[step, c], tr_sem.at[step, c], base + to
            ).start()
            return carry

        lax.fori_loop(1, group, send, 0)
        in_t[c, slab] = out_t[c, which, seat]

    def drain(view, sem):
        pltpu.make_async_copy(view, view, sem).wait()

    def forward_yx(step, c):
        drain(in_t.at[c, pl.ds(0, n - 2)], tr_sem.at[step, c])
        parts = [in_t[c, :, part].reshape(cells_x * kz_own, cells_y) for part in range(2)]
        dims = (((1,), (0,)), ((), ()))
        res = three_pass(split(jnp.concatenate(parts, axis=1)), (wy_h[...], wy_l[...]), dims)
        for part in range(2):
            for h in range(halves):
                at = part * padded_y + h * 128
                piece = res[:, at:at + 128].reshape(cells_x, kz_own, 128)
                for j in range(chunks):
                    lines[j * halves + h, part] = piece[:, j * kc:(j + 1) * kc]

        def columns(i, carry):
            line = [(lines[i, 0, x], lines[i, 1, x]) for x in range(cells_x)]
            for m, (re, im) in enumerate(fft(line, -1)):
                spec[i, 2 * c, 2 * m], spec[i, 2 * c + 1, 2 * m] = re, im
            line = [twiddle(lines[i, 0, x], lines[i, 1, x], x, padded_x, -1) for x in range(cells_x)]
            for m, (re, im) in enumerate(fft(line, -1)):
                spec[i, 2 * c, 2 * m + 1], spec[i, 2 * c + 1, 2 * m + 1] = re, im
            return carry

        lax.fori_loop(0, chunks * halves, columns, 0)

    def backward_xy(step, a):
        row = COMBOS[a]

        def columns(i, carry):
            def field(k):
                g = [green[i, r, k] for r in row]
                s = [spec[i, r, k] for r in range(6)]
                return g[0] * s[0] + g[1] * s[2] + g[2] * s[4], g[0] * s[1] + g[1] * s[3] + g[2] * s[5]

            even = fft([field(k) for k in range(0, padded_x, 2)], 1)
            for x in range(cells_x):
                lines[i, 0, x], lines[i, 1, x] = even[x]
            odd = fft([field(k) for k in range(1, padded_x, 2)], 1)
            for x in range(cells_x):
                re, im = twiddle(*odd[x], x, padded_x, 1)
                lines[i, 0, x] += re
                lines[i, 1, x] += im
            return carry

        lax.fori_loop(0, chunks * halves, columns, 0)
        parts = []
        for part in range(2):
            for h in range(halves):
                pieces = [lines[j * halves + h, part] for j in range(chunks)]
                piece = pieces[0] if chunks == 1 else jnp.concatenate(pieces, axis=1)
                parts.append(piece.reshape(cells_x * kz_own, 128))
        dims = (((1,), (0,)), ((), ()))
        res = three_pass(split(jnp.concatenate(parts, axis=1)), (vy_h[...], vy_l[...]), dims)
        for part in range(2):
            piece = res[:, part * cells_y:(part + 1) * cells_y]
            out_u[a, :, part] = piece.reshape(cells_x, kz_own, cells_y)
        send_back(step, a, 1, (1 - here) * group, cs_sem, cr_sem)
        send_back(step, a, 0, base, os_sem, or_sem)

    def send_back(step, a, which, first, s_sem, r_sem):
        def send(k, carry):
            to = lax.rem(seat + k, group)
            remote(
                out_u.at[a, first + to], in_u.at[a, which, seat], s_sem.at[step, a], r_sem.at[step, a], base + to
            ).start()
            return carry

        lax.fori_loop(1, group, send, 0)
        in_u[a, which, seat] = out_u[a, first + seat]

    def inverse_z(a, which):
        total = None
        for part in range(2):
            field = in_u[a, which, :, part].reshape(kz_half, cells_y)
            dims = (((0,), (0,)), ((), ()))
            term = three_pass(split(field), (vz_h[here, part], vz_l[here, part]), dims)
            total = term if total is None else total + term
        return total

    def send_part(step, a):
        drain(in_u.at[a, 1, pl.ds(0, group - 1)], cr_sem.at[step, a])
        part_out[a] = inverse_z(a, 1)
        remote(part_out.at[a], part_in.at[a], ps_sem.at[step, a], pr_sem.at[step, a], twin).start()

    for step in range(MATVECS):
        source, image = (pol_ref, first_ref) if step == 0 else (first_ref, second_ref)
        if step == 0:
            pl.semaphore_wait(barrier, group)
            for c in range(3):
                send_raw(step, c, source[c, 0] * mask_ref[...])
            for c in range(3):
                forward_z(step, c, 0, raw_out[c])
            order_green()
        for c in range(3):
            drain(raw_in.at[c], wr_sem.at[step, c])
            forward_z(step, c, 1, raw_in[c])
            if c > 0:
                forward_yx(step, c - 1)
        forward_yx(step, 2)
        for a in range(3):
            backward_xy(step, a)
            if a > 0:
                send_part(step, a - 1)
        send_part(step, 2)
        for c in range(3):
            drain(raw_out.at[c], ws_sem.at[step, c])
            drain(in_t.at[c, pl.ds(0, n - 2)], ts_sem.at[step, c])
        for a in range(3):
            drain(in_u.at[a, 0, pl.ds(0, group - 1)], or_sem.at[step, a])
            own = inverse_z(a, 0)
            masked = source[a, 0] * mask_ref[...]
            drain(part_in.at[a], pr_sem.at[step, a])
            image[a, 0] = inv_ref[0] * masked - mask_ref[...] * (own + part_in[a])
            if step + 1 < MATVECS:
                send_raw(step + 1, a, image[a, 0] * mask_ref[...])
                forward_z(step + 1, a, 0, raw_out[a])
        for a in range(3):
            drain(in_u.at[a, 1, pl.ds(0, group - 1)], cs_sem.at[step, a])
            drain(in_u.at[a, 0, pl.ds(0, group - 1)], os_sem.at[step, a])
            drain(part_out.at[a], ps_sem.at[step, a])


def deliver(first_ref, second_ref, first_out, second_out, first, second, in_sem, out_sem):
    loads = [
        pltpu.make_async_copy(source, held, in_sem.at[i])
        for i, (source, held) in enumerate(((first_ref, first), (second_ref, second)))
    ]
    stores = [
        pltpu.make_async_copy(held, target, out_sem.at[i])
        for i, (held, target) in enumerate(((first, first_out), (second, second_out)))
    ]
    for copy in loads:
        copy.start()
    for load, store in zip(loads, stores):
        load.wait()
        store.start()
    for store in stores:
        store.wait()


def per_device(n, polarization, inverse_polarizability, occupancy, green_fourier):
    _, _, cells_y, cells_z = polarization.shape
    _, kz_own, padded_x, padded_y = green_fourier.shape
    padded_z = 2 * cells_z
    cells_x = padded_x // 2
    kc = min(8, kz_own)
    chunks = kz_own // kc
    halves = padded_y // 128
    cos, sin = tables(padded_z, cells_z, padded_z)
    wz = split_table(np.stack([cos, -sin]).reshape(2, 2, cells_z, cells_z).swapaxes(0, 1))
    cos, sin = tables(cells_y, padded_y, padded_y)
    wy = split_table(np.block([[cos, -sin], [sin, cos]]))
    cos, sin = tables(padded_y, cells_y, padded_y)
    vy = split_table(np.block([[cos, sin], [-sin, cos]]))
    cos, sin = tables(padded_z, cells_z, padded_z)
    vz = np.stack([cos, -sin]).reshape(2, 2, cells_z, cells_z).swapaxes(0, 1)
    vz = split_table(vz / (padded_x * padded_y * padded_z))
    vmem = pl.BlockSpec(memory_space=pltpu.VMEM)
    images = pl.pallas_call(
        functools.partial(kernel, n, cells_x, padded_x, kz_own, kc),
        out_shape=(jax.ShapeDtypeStruct(polarization.shape, F32),) * 2,
        in_specs=[vmem] * 3 + [pl.BlockSpec(memory_space=pl.ANY)] + [vmem] * 8,
        out_specs=(vmem, vmem),
        scratch_shapes=[
            pltpu.VMEM(green_fourier.shape, F32),
            pltpu.VMEM((chunks * halves, 6, padded_x, kc, 128), F32),
            pltpu.VMEM((cells_y, cells_z), F32),
            pltpu.VMEM((3, cells_y, cells_z), F32),
            pltpu.VMEM((3, cells_y, cells_z), F32),
            pltpu.VMEM((3, 2, n // 2, 2, kz_own, cells_y), F32),
            pltpu.VMEM((3, n, 2, kz_own, cells_y), F32),
            pltpu.VMEM((chunks * halves, 2, cells_x, kc, 128), F32),
            pltpu.VMEM((chunks * halves, 6, padded_x, kc, 128), F32),
            pltpu.VMEM((3, n, 2, kz_own, cells_y), F32),
            pltpu.VMEM((3, 2, n // 2, 2, kz_own, cells_y), F32),
            pltpu.VMEM((3, cells_y, cells_z), F32),
            pltpu.VMEM((3, cells_y, cells_z), F32),
            pltpu.SemaphoreType.DMA,
            *[pltpu.SemaphoreType.DMA((MATVECS, 3))] * 10,
        ],
        compiler_params=pltpu.CompilerParams(
            collective_id=0, has_side_effects=True, vmem_limit_bytes=60 * 1024 * 1024
        ),
    )(polarization, inverse_polarizability, occupancy, green_fourier, *map(jnp.asarray, wz + wy + vy + vz))
    anywhere = pl.BlockSpec(memory_space=pl.ANY)
    return pl.pallas_call(
        deliver,
        out_shape=(jax.ShapeDtypeStruct(polarization.shape, F32),) * 2,
        in_specs=[anywhere] * 2,
        out_specs=(anywhere, anywhere),
        scratch_shapes=[pltpu.VMEM(polarization.shape, F32)] * 2 + [pltpu.SemaphoreType.DMA((2,))] * 2,
    )(*images)


def solution(mesh):
    return jax.shard_map(
        functools.partial(per_device, mesh.shape["slab"]),
        mesh=mesh,
        in_specs=(
            P("comp", "slab", None, None),
            P("slab", None, None),
            P("slab", None, None),
            P(None, "slab", None, None),
        ),
        out_specs=(P("comp", "slab", None, None), P("comp", "slab", None, None)),
        check_vma=False,
    )
```
